32 devices in a mesh: dp: 8 (over z, x), mp: 4 (over y, core).
Axes of the slice: x: 2, y: 2, z: 4, core: 2. Of those that a mesh axis runs over, the one named last changes fastest.
Arguments:
- hidden: bfloat16 [8, 512, 4608], P('dp', 'mp'), may hold values from -6 to 6
- lengths: int32 [8], P('dp'), may hold values from 64 to 512
- norm_gain: float32 [4608], replicated, may hold values from 0.25 to 1.75
- w_query: bfloat16 [4608, 2048], P('dp', 'mp'), may hold values from -0.09375 to 0.09375
- w_key: bfloat16 [4608, 1024], P('dp', 'mp'), may hold values from -0.09375 to 0.09375
- w_value: bfloat16 [4608, 1024], P('dp', 'mp'), may hold values from -0.09375 to 0.09375
- w_out: bfloat16 [2048, 4608], P('mp', 'dp'), may hold values from -0.125 to 0.125
- post_gain: float32 [4608], replicated, may hold values from 0.25 to 1.75
Outputs:
- mixed: bfloat16 [8, 512, 4608], P('dp', 'mp')
- key_cache: bfloat16 [8, 512, 1024], P('dp', None, 'mp')
- value_cache: bfloat16 [8, 512, 1024], P('dp', None, 'mp')
The draws below stay inside these ranges and needn't reach their ends.
All inputs are finite; a program needn't handle non-finite values.
Results may differ from the reference program's by a relative error of at most 0.01.
Values may be sent and summed in bfloat16 or wider, within the bound.
A program may use at most 128 MiB of HBM per device.

```python
import jax
import jax.numpy as jnp
from jax import lax

D = 4608
HD = 128
QH = 16
KVH = 8
MAXLEN = 512
MINLEN = 64
ROLLOUTS = 8
N_MP = 4


def place_ends(values, key, low, largest):
    spot = [jax.random.randint(jax.random.fold_in(key, axis), (), 0, length) for axis, length in enumerate(values.shape)]
    widest = values.shape.index(max(values.shape))
    beside = spot[:widest] + [(spot[widest] + 1) % values.shape[widest]] + spot[widest + 1:]
    return values.at[tuple(spot)].set(low).at[tuple(beside)].set(largest)


def block_levels(own_key, shape, pieces, least, largest):
    level, own = 1.0, jax.random.fold_in(own_key, 6)
    for position, shards_of in pieces:
        steps = jnp.exp(jax.random.uniform(jax.random.fold_in(own, position), (shards_of,), jnp.float32, least / len(pieces), largest / len(pieces)))
        level = level * jnp.repeat(steps, shape[position] // shards_of).reshape([-1 if axis == position else 1 for axis in range(len(shape))])
    return level


def centred(stream_key, shape, scale, limit, cuts=(), kind=jnp.bfloat16):
    result = scale * jax.random.normal(stream_key, shape, jnp.float32)
    if cuts:
        result = result * block_levels(stream_key, shape, cuts, -0.22, 0.18)
    return jnp.clip(result, -limit, limit).astype(kind)


def setup_inputs(seed: int = 0) -> dict:
    seeds = jax.random.split(jax.random.key(seed), 9)
    hidden = centred(seeds[0], (ROLLOUTS, MAXLEN, D), 1.0, 6.0, ((0, 8), (1, 4)))
    lengths = place_ends(jax.random.randint(seeds[1], (ROLLOUTS,), MINLEN, MAXLEN + 1), jax.random.fold_in(seeds[1], 1), MINLEN, MAXLEN).astype(jnp.int32)
    norm_gain = jnp.clip(1.0 + 0.15 * jax.random.normal(seeds[2], (D,), jnp.float32), 0.25, 1.75)
    w_query = centred(seeds[3], (D, QH * HD), D ** -0.5, 0.09375, ((0, 8), (1, 4)))
    w_key = centred(seeds[4], (D, KVH * HD), D ** -0.5, 0.09375, ((0, 8), (1, 4)))
    w_value = centred(seeds[5], (D, KVH * HD), D ** -0.5, 0.09375, ((0, 8), (1, 4)))
    w_out = centred(seeds[6], (QH * HD, D), (QH * HD) ** -0.5, 0.125, ((0, 4), (1, 8)))
    post_gain = jnp.clip(1.0 + 0.15 * jax.random.normal(seeds[7], (D,), jnp.float32), 0.25, 1.75)
    return {"hidden": hidden, "lengths": lengths, "norm_gain": norm_gain, "w_query": w_query, "w_key": w_key, "w_value": w_value, "w_out": w_out, "post_gain": post_gain}


def rotate(values, positions):
    half = values.shape[-1] // 2
    freqs = 10000.0 ** (-jnp.arange(half, dtype=jnp.float32) / half)
    angles = positions.astype(jnp.float32)[:, None] * freqs[None, :]
    cosine = jnp.cos(angles)[:, None, :]
    sine = jnp.sin(angles)[:, None, :]
    first = values[..., :half]
    second = values[..., half:]
    return jnp.concatenate([first * cosine - second * sine, second * cosine + first * sine], axis=-1)

def one_rollout(args, norm_gain, w_query, w_key, w_value, w_out, post_gain):
    rows, length = args
    maxlen = rows.shape[0]
    group = QH // KVH
    rows_f = rows.astype(jnp.float32)
    normed = (rows_f * lax.rsqrt(lax.optimization_barrier(jnp.mean(rows_f * rows_f, axis=-1, keepdims=True)) + 1e-06) * norm_gain).astype(jnp.bfloat16)
    positions = jnp.arange(maxlen, dtype=jnp.int32)
    qraw = jnp.dot(normed, w_query, preferred_element_type=jnp.float32).reshape(maxlen, QH, HD)
    kraw = jnp.dot(normed, w_key, preferred_element_type=jnp.float32).reshape(maxlen, KVH, HD)
    vraw = jnp.dot(normed, w_value, preferred_element_type=jnp.float32).reshape(maxlen, KVH, HD)
    query = (rotate(qraw, positions) * 144.0 ** (-0.5)).astype(jnp.bfloat16)
    key = rotate(kraw, positions).astype(jnp.bfloat16)
    value = vraw.astype(jnp.bfloat16)
    grouped = query.reshape(maxlen, KVH, group, HD).astype(jnp.float32)
    score = jnp.einsum('qkgd,tkd->kgqt', grouped, key.astype(jnp.float32))
    score = 50.0 * jnp.tanh(score / 50.0)
    keep = (positions[None, :] <= positions[:, None]) & (positions[None, :] < length)
    score = jnp.where(keep[None, None], score, -1e+30)
    top = lax.optimization_barrier(jnp.max(score, axis=-1, keepdims=True))
    expo = jnp.exp(score - top)
    weights = (expo / lax.optimization_barrier(jnp.sum(expo, axis=-1, keepdims=True))).astype(jnp.bfloat16)
    attended = jnp.einsum('kgqt,tkd->qkgd', weights.astype(jnp.float32), value.astype(jnp.float32))
    attended = attended.reshape(maxlen, QH * HD).astype(jnp.bfloat16)
    cols = QH * HD // N_MP
    projected = jnp.zeros((maxlen, D), jnp.float32)
    for part in range(N_MP):
        partial_value = jnp.dot(attended[:, part * cols:(part + 1) * cols], w_out[part * cols:(part + 1) * cols], preferred_element_type=jnp.float32)
        projected = projected + partial_value.astype(jnp.bfloat16).astype(jnp.float32)
    post = projected * lax.rsqrt(lax.optimization_barrier(jnp.mean(projected * projected, axis=-1, keepdims=True)) + 1e-06) * post_gain
    live = (positions < length)[:, None]
    mixed = jnp.where(live, rows_f + post, 0.0).astype(jnp.bfloat16)
    key_rows = jnp.where(live, key.reshape(maxlen, KVH * HD), jnp.zeros((), jnp.bfloat16))
    value_rows = jnp.where(live, value.reshape(maxlen, KVH * HD), jnp.zeros((), jnp.bfloat16))
    return (mixed, key_rows, value_rows)

def reference(hidden, lengths, norm_gain, w_query, w_key, w_value, w_out, post_gain):

    def step(args):
        return one_rollout(args, norm_gain, w_query, w_key, w_value, w_out, post_gain)
    mixed, key_cache, value_cache = lax.map(step, (hidden, lengths))
    return (mixed, key_cache, value_cache)
```

```python
import functools

import jax
import jax.numpy as jnp
import numpy as np
from jax import lax
from jax.experimental import pallas as pl
from jax.experimental.pallas import tpu as pltpu
from jax.sharding import PartitionSpec as P

HD = 128
MESH = pl.DeviceIdType.MESH
UP, DOWN, ACROSS = 0, 1, 2


def tables(maxlen):
    half = HD // 2
    freqs = 10000.0 ** (-np.arange(half, dtype=np.float64) / half)
    angles = np.arange(maxlen, dtype=np.float64)[:, None] * freqs[None, :]
    cosine, sine = np.cos(angles), np.sin(angles)
    return (
        np.concatenate([cosine, cosine], axis=1).astype(np.float32),
        np.concatenate([-sine, sine], axis=1).astype(np.float32),
    )


def cut(rows):
    if rows % 32:
        return [None, (0, rows)]
    first = rows // 6 // 16 * 16
    rest = rows - first
    chunk = rest // 2 // 16 * 16
    return [(0, first), (first, chunk), (first + chunk, rest - chunk)]


def kernel(
    n_dp, n_mp, cuts,
    len_ref, hid, ngain, wq, wk, wv, wo, pgain, cos_ref, sin_ref,
    mixed, key_out, val_out,
    wbuf, obuf, nbuf, acc, att, psend, precv,
    load_sem, send_sem, recv_sem, nsend_sem, nrecv_sem, psend_sem, precv_sem,
):
    nz = n_dp // 2
    me, mp = lax.axis_index("dp"), lax.axis_index("mp")
    z, x = me // 2, me % 2
    local_len, width = hid.shape
    maxlen = local_len * n_mp
    fcols = width // n_dp
    qw, kw = wq.shape[1], wk.shape[1]
    q_heads, kv_heads = qw // HD, kw // HD
    can_up, can_down = z < nz - 1, z > 0
    bufs = (wbuf, obuf)

    loads = [
        pltpu.make_async_copy(wq, wbuf.at[me, :, pl.ds(0, qw)], load_sem.at[0]),
        pltpu.make_async_copy(wk, wbuf.at[me, :, pl.ds(qw, kw)], load_sem.at[1]),
        pltpu.make_async_copy(wv, wbuf.at[me, :, pl.ds(qw + kw, kw)], load_sem.at[2]),
        pltpu.make_async_copy(wo, obuf.at[me], load_sem.at[3]),
    ]
    for load in loads:
        load.start()

    barrier = pltpu.get_barrier_semaphore()

    def greet(dp_index, mp_index):
        pl.semaphore_signal(barrier, inc=1, device_id=(dp_index, mp_index), device_id_type=MESH)

    greet(me + 1 - 2 * x, mp)
    for step in range(1, n_mp):
        greet(me, lax.rem(mp + step, n_mp))

    @pl.when(can_up)
    def _():
        greet(me + 2, mp)

    @pl.when(can_down)
    def _():
        greet(me - 2, mp)

    pl.semaphore_wait(
        barrier, n_mp + jnp.where(can_up, 1, 0) + jnp.where(can_down, 1, 0)
    )

    def copy(kind, part, origin, way):
        start, size = cuts[kind][part]
        ref = bufs[kind].at[origin, pl.ds(start, size)]
        target = (me + 2, me - 2, me + 1 - 2 * x)[way]
        return pltpu.make_async_remote_copy(
            src_ref=ref,
            dst_ref=ref,
            send_sem=send_sem.at[kind, part, way, origin],
            recv_sem=recv_sem.at[kind, part, origin],
            device_id=(target, mp),
            device_id_type=MESH,
        )

    def send_chain(kind, part, origin):
        @pl.when(can_up)
        def _():
            copy(kind, part, origin, UP).start()

        @pl.when(can_down)
        def _():
            copy(kind, part, origin, DOWN).start()

    def rest_of(kind):
        return range(1, len(cuts[kind]))

    def send_own(kind):
        if cuts[kind][0]:
            copy(kind, 0, me, ACROSS).start()
        for part in rest_of(kind):
            send_chain(kind, part, me)
            copy(kind, part, me, ACROSS).start()
        if cuts[kind][0]:
            send_chain(kind, 0, me)

    def send_partner(kind):
        if cuts[kind][0]:
            partner = me + 1 - 2 * x
            copy(kind, 0, partner, ACROSS).wait_recv()
            send_chain(kind, 0, partner)

    def relay(kind, k):
        below, above = z - k, z + k
        for part in rest_of(kind):
            @pl.when(below >= 0)
            def _():
                origin = below * 2 + x
                copy(kind, part, origin, UP).wait_recv()

                @pl.when(can_up)
                def _():
                    copy(kind, part, origin, UP).start()

                copy(kind, part, origin, ACROSS).start()

            @pl.when(above < nz)
            def _():
                origin = above * 2 + x
                copy(kind, part, origin, DOWN).wait_recv()

                @pl.when(can_down)
                def _():
                    copy(kind, part, origin, DOWN).start()

                copy(kind, part, origin, ACROSS).start()

        if cuts[kind][0]:
            for column in range(2):
                @pl.when(below >= 0)
                def _():
                    origin = below * 2 + column
                    copy(kind, 0, origin, UP).wait_recv()

                    @pl.when(can_up)
                    def _():
                        copy(kind, 0, origin, UP).start()

                @pl.when(above < nz)
                def _():
                    origin = above * 2 + column
                    copy(kind, 0, origin, DOWN).wait_recv()

                    @pl.when(can_down)
                    def _():
                        copy(kind, 0, origin, DOWN).start()

    def wait_across(kind, origin):
        for part in rest_of(kind):
            copy(kind, part, origin, ACROSS).wait_recv()

    def drain(kind):
        def body(origin, carry):
            oz, ox = origin // 2, origin % 2
            for part in range(len(cuts[kind])):
                if not cuts[kind][part]:
                    continue
                mine = (ox == x) | (part == 0)

                @pl.when(mine & (oz <= z) & can_up)
                def _():
                    copy(kind, part, origin, UP).wait_send()

                @pl.when(mine & (oz >= z) & can_down)
                def _():
                    copy(kind, part, origin, DOWN).wait_send()

                @pl.when((origin == me) if part == 0 else (ox == x))
                def _():
                    copy(kind, part, origin, ACROSS).wait_send()

            return carry

        lax.fori_loop(0, n_dp, body, 0)

    for load in loads[:3]:
        load.wait()
    send_own(0)

    total = jnp.zeros((local_len, 1), jnp.float32)
    for block in range(n_dp):
        rows = hid[:, block * fcols : (block + 1) * fcols].astype(jnp.float32)
        total = total + jnp.sum(rows * rows, axis=-1, keepdims=True)
    scale = lax.rsqrt(total / width + 1e-06)
    for block in range(n_dp):
        span = slice(block * fcols, (block + 1) * fcols)
        rows = hid[:, span].astype(jnp.float32)
        nbuf[mp, block] = (rows * scale * ngain[:, span]).astype(jnp.bfloat16)

    def share(step):
        return pltpu.make_async_remote_copy(
            src_ref=nbuf.at[mp],
            dst_ref=nbuf.at[mp],
            send_sem=nsend_sem.at[step],
            recv_sem=nrecv_sem.at[mp],
            device_id=(me, lax.rem(mp + step, n_mp)),
            device_id_type=MESH,
        )

    def shared(source):
        return pltpu.make_async_remote_copy(
            src_ref=nbuf.at[source],
            dst_ref=nbuf.at[source],
            send_sem=nsend_sem.at[0],
            recv_sem=nrecv_sem.at[source],
            device_id=(me, source),
            device_id_type=MESH,
        )

    for step in range(1, n_mp):
        share(step).start()
    send_partner(0)
    acc[...] = jnp.zeros_like(acc)

    def step_qkv(k, carry):
        relay(0, k)
        return carry

    lax.fori_loop(1, nz, step_qkv, 0)
    loads[3].wait()
    send_own(1)
    for step in range(1, n_mp):
        shared(lax.rem(mp + step, n_mp)).wait_recv()

    def project(i, carry):
        other, k, side = i // (2 * nz), i // 2 % nz, i % 2
        oz = z + k * (2 * side - 1)
        origin = oz * 2 + lax.rem(x + other, 2)

        @pl.when((oz >= 0) & (oz < nz) & ((side == 0) | (k > 0)))
        def _():
            @pl.when(other == 1)
            def _():
                wait_across(0, origin)

            for m in range(n_mp):
                span = slice(m * local_len, (m + 1) * local_len)
                acc[span, :] += jnp.dot(
                    nbuf[m, origin], wbuf[origin], preferred_element_type=jnp.float32
                )

        return carry

    lax.fori_loop(0, 4 * nz, project, 0)
    send_partner(1)

    length = len_ref[0]
    live = lax.broadcasted_iota(jnp.int32, (maxlen, HD), 0) < length

    def rotated(block, span):
        return block * cos_ref[span, :] + pltpu.roll(block, HD // 2, 1) * sin_ref[span, :]

    everything = slice(0, maxlen)
    for h in range(kv_heads):
        cols = slice(h * HD, (h + 1) * HD)
        keys = rotated(acc[:, qw + h * HD : qw + (h + 1) * HD], everything)
        key_out[:, cols] = jnp.where(live, keys, 0.0).astype(jnp.bfloat16)
        values = acc[:, qw + kw + h * HD : qw + kw + (h + 1) * HD]
        val_out[:, cols] = jnp.where(live, values, 0.0).astype(jnp.bfloat16)
    for h in range(q_heads):
        kv = h * kv_heads // q_heads
        cols = slice(kv * HD, (kv + 1) * HD)
        for r in range(n_mp):
            span, seen = slice(r * local_len, (r + 1) * local_len), (r + 1) * local_len
            query = rotated(acc[span, h * HD : (h + 1) * HD], span) * 144.0 ** (-0.5)
            score = lax.dot_general(
                query.astype(jnp.bfloat16),
                key_out[:seen, cols],
                (((1,), (1,)), ((), ())),
                preferred_element_type=jnp.float32,
            )
            row = lax.broadcasted_iota(jnp.int32, score.shape, 0) + r * local_len
            col = lax.broadcasted_iota(jnp.int32, score.shape, 1)
            expo = jnp.exp(50.0 * jnp.tanh(score * (1.0 / 50.0)))
            expo = jnp.where((col <= row) & (col < length), expo, 0.0)
            weights = (expo / jnp.sum(expo, axis=-1, keepdims=True)).astype(jnp.bfloat16)
            att[span, h * HD : (h + 1) * HD] = jnp.dot(
                weights, val_out[:seen, cols], preferred_element_type=jnp.float32
            ).astype(jnp.bfloat16)

    def hand(block, step):
        target = lax.rem(mp + step, n_mp)
        return pltpu.make_async_remote_copy(
            src_ref=psend.at[block, target],
            dst_ref=precv.at[block, n_mp - 1 - step],
            send_sem=psend_sem.at[block, n_mp - 1 - step],
            recv_sem=precv_sem.at[block, n_mp - 1 - step],
            device_id=(me, target),
            device_id_type=MESH,
        )

    def output(block):
        for m in range(n_mp):
            span = slice(m * local_len, (m + 1) * local_len)
            psend[block, m] = jnp.dot(
                att[span, :], obuf[block], preferred_element_type=jnp.float32
            ).astype(jnp.bfloat16)
        for step in range(1, n_mp):
            hand(block, step).start()

    def step_out(k, carry):
        @pl.when((k > 0) & (k < nz))
        def _():
            relay(1, k)

        def each(i, inner):
            other, side = i // 2, i % 2
            distance = k - other
            oz = z + distance * (2 * side - 1)
            origin = oz * 2 + lax.rem(x + other, 2)

            @pl.when(
                (distance >= 0) & (distance < nz) & (oz >= 0) & (oz < nz)
                & ((side == 0) | (distance > 0))
            )
            def _():
                @pl.when(other == 1)
                def _():
                    wait_across(1, origin)

                output(origin)

            return inner

        return lax.fori_loop(0, 4, each, carry)

    lax.fori_loop(0, nz + 1, step_out, 0)

    def summed(block):
        value = psend[block, mp].astype(jnp.float32)
        for slot in range(n_mp - 1):
            value = value + precv[block, slot].astype(jnp.float32)
        return value

    def squares(block, total):
        for step in range(1, n_mp):
            hand(block, step).wait_recv()
        value = summed(block)
        return total + jnp.sum(value * value, axis=-1, keepdims=True)

    total = lax.fori_loop(0, n_dp, squares, jnp.zeros((local_len, 1), jnp.float32))
    scale = lax.rsqrt(total / width + 1e-06)
    own = lax.broadcasted_iota(jnp.int32, (local_len, fcols), 0) + mp * local_len < length
    for block in range(n_dp):
        span = slice(block * fcols, (block + 1) * fcols)
        post = summed(block) * scale * pgain[:, span]
        mixed[:, span] = jnp.where(own, hid[:, span].astype(jnp.float32) + post, 0.0).astype(
            jnp.bfloat16
        )

    drain(0)
    drain(1)
    for step in range(1, n_mp):
        share(step).wait_send()

    def drain_hand(block, carry):
        for step in range(1, n_mp):
            hand(block, step).wait_send()
        return carry

    lax.fori_loop(0, n_dp, drain_hand, 0)


def local(n_dp, n_mp, hidden, lengths, norm_gain, w_query, w_key, w_value, w_out, post_gain):
    _, local_len, width = hidden.shape
    maxlen = local_len * n_mp
    rows, qw = w_query.shape
    kw = w_key.shape[1]
    orows, fcols = w_out.shape
    cuts = (cut(rows), cut(orows))
    cosine, sine = tables(maxlen)
    vmem = pl.BlockSpec(memory_space=pltpu.VMEM)
    anywhere = pl.BlockSpec(memory_space=pl.ANY)
    bf16, f32 = jnp.bfloat16, jnp.float32
    dma = pltpu.SemaphoreType.DMA
    mixed, keys, values = pl.pallas_call(
        functools.partial(kernel, n_dp, n_mp, cuts),
        out_shape=(
            jax.ShapeDtypeStruct((local_len, width), bf16),
            jax.ShapeDtypeStruct((maxlen, kw), bf16),
            jax.ShapeDtypeStruct((maxlen, kw), bf16),
        ),
        in_specs=[pl.BlockSpec(memory_space=pltpu.SMEM), vmem, vmem]
        + [anywhere] * 4
        + [vmem, vmem, vmem],
        out_specs=(vmem, vmem, vmem),
        scratch_shapes=[
            pltpu.VMEM((n_dp, rows, qw + 2 * kw), bf16),
            pltpu.VMEM((n_dp, orows, fcols), bf16),
            pltpu.VMEM((n_mp, n_dp, local_len, fcols), bf16),
            pltpu.VMEM((maxlen, qw + 2 * kw), f32),
            pltpu.VMEM((maxlen, qw), bf16),
            pltpu.VMEM((n_dp, n_mp, local_len, fcols), bf16),
            pltpu.VMEM((n_dp, n_mp - 1, local_len, fcols), bf16),
            dma((4,)),
            dma((2, 3, 3, n_dp)),
            dma((2, 3, n_dp)),
            dma((n_mp,)),
            dma((n_mp,)),
            dma((n_dp, n_mp - 1)),
            dma((n_dp, n_mp - 1)),
        ],
        compiler_params=pltpu.CompilerParams(
            collective_id=0, has_side_effects=True, vmem_limit_bytes=60 * 1024 * 1024
        ),
    )(
        lengths,
        hidden[0],
        norm_gain.reshape(1, width),
        w_query,
        w_key,
        w_value,
        w_out,
        post_gain.reshape(1, width),
        jnp.asarray(cosine),
        jnp.asarray(sine),
    )
    return mixed[None], keys[None], values[None]


def solution(mesh):
    return jax.shard_map(
        functools.partial(local, mesh.shape["dp"], mesh.shape["mp"]),
        mesh=mesh,
        in_specs=(
            P("dp", "mp", None),
            P("dp"),
            P(),
            P("dp", "mp"),
            P("dp", "mp"),
            P("dp", "mp"),
            P("mp", "dp"),
            P(),
        ),
        out_specs=(P("dp", "mp", None), P("dp", None, "mp"), P("dp", None, "mp")),
        check_vma=False,
    )
```

```python
import functools

import jax
import jax.numpy as jnp
import numpy as np
from jax import lax
from jax.experimental import pallas as pl
from jax.experimental.pallas import tpu as pltpu
from jax.sharding import PartitionSpec as P

HD = 128
MESH = pl.DeviceIdType.MESH
UP, DOWN, ACROSS = 0, 1, 2


def tables(maxlen):
    half = HD // 2
    freqs = 10000.0 ** (-np.arange(half, dtype=np.float64) / half)
    angles = np.arange(maxlen, dtype=np.float64)[:, None] * freqs[None, :]
    cosine, sine = np.cos(angles), np.sin(angles)
    return (
        np.concatenate([cosine, cosine], axis=1).astype(np.float32),
        np.concatenate([-sine, sine], axis=1).astype(np.float32),
    )


def cut(rows):
    if rows % 32:
        return [None, (0, rows)]
    first = rows // 6 // 16 * 16
    rest = rows - first
    chunk = rest // 2 // 16 * 16
    return [(0, first), (first, chunk), (first + chunk, rest - chunk)]


def kernel(
    n_dp, n_mp, cuts,
    len_ref, hid, ngain, wq, wk, wv, wo, pgain, cos_ref, sin_ref,
    mixed, key_out, val_out,
    wbuf, obuf, nbuf, acc, att, psend, precv,
    load_sem, send_sem, recv_sem, nsend_sem, nrecv_sem, psend_sem, precv_sem,
):
    nz = n_dp // 2
    me, mp = lax.axis_index("dp"), lax.axis_index("mp")
    z, x = me // 2, me % 2
    local_len, width = hid.shape
    maxlen = local_len * n_mp
    fcols = width // n_dp
    qw, kw = wq.shape[1], wk.shape[1]
    q_heads, kv_heads = qw // HD, kw // HD
    can_up, can_down = z < nz - 1, z > 0
    bufs = (wbuf, obuf)

    loads = [
        pltpu.make_async_copy(wq, wbuf.at[me, :, pl.ds(0, qw)], load_sem.at[0]),
        pltpu.make_async_copy(wk, wbuf.at[me, :, pl.ds(qw, kw)], load_sem.at[1]),
        pltpu.make_async_copy(wv, wbuf.at[me, :, pl.ds(qw + kw, kw)], load_sem.at[2]),
        pltpu.make_async_copy(wo, obuf.at[me], load_sem.at[3]),
    ]
    for load in loads:
        load.start()

    barrier = pltpu.get_barrier_semaphore()

    def greet(dp_index, mp_index):
        pl.semaphore_signal(barrier, inc=1, device_id=(dp_index, mp_index), device_id_type=MESH)

    greet(me + 1 - 2 * x, mp)
    for step in range(1, n_mp):
        greet(me, lax.rem(mp + step, n_mp))

    @pl.when(can_up)
    def _():
        greet(me + 2, mp)

    @pl.when(can_down)
    def _():
        greet(me - 2, mp)

    pl.semaphore_wait(
        barrier, n_mp + jnp.where(can_up, 1, 0) + jnp.where(can_down, 1, 0)
    )

    def copy(kind, part, origin, way):
        start, size = cuts[kind][part]
        ref = bufs[kind].at[origin, pl.ds(start, size)]
        target = (me + 2, me - 2, me + 1 - 2 * x)[way]
        return pltpu.make_async_remote_copy(
            src_ref=ref,
            dst_ref=ref,
            send_sem=send_sem.at[kind, part, way, origin],
            recv_sem=recv_sem.at[kind, part, origin],
            device_id=(target, mp),
            device_id_type=MESH,
        )

    def send_chain(kind, part, origin):
        @pl.when(can_up)
        def _():
            copy(kind, part, origin, UP).start()

        @pl.when(can_down)
        def _():
            copy(kind, part, origin, DOWN).start()

    def rest_of(kind):
        return range(1, len(cuts[kind]))

    def send_own(kind):
        if cuts[kind][0]:
            copy(kind, 0, me, ACROSS).start()
        for part in rest_of(kind):
            send_chain(kind, part, me)
            copy(kind, part, me, ACROSS).start()
        if cuts[kind][0]:
            send_chain(kind, 0, me)

    def send_partner(kind):
        if cuts[kind][0]:
            partner = me + 1 - 2 * x
            copy(kind, 0, partner, ACROSS).wait_recv()
            send_chain(kind, 0, partner)

    def relay(kind, k):
        below, above = z - k, z + k
        for part in rest_of(kind):
            @pl.when(below >= 0)
            def _():
                origin = below * 2 + x
                copy(kind, part, origin, UP).wait_recv()

                @pl.when(can_up)
                def _():
                    copy(kind, part, origin, UP).start()

                copy(kind, part, origin, ACROSS).start()

            @pl.when(above < nz)
            def _():
                origin = above * 2 + x
                copy(kind, part, origin, DOWN).wait_recv()

                @pl.when(can_down)
                def _():
                    copy(kind, part, origin, DOWN).start()

                copy(kind, part, origin, ACROSS).start()

        if cuts[kind][0]:
            for column in range(2):
                @pl.when(below >= 0)
                def _():
                    origin = below * 2 + column
                    copy(kind, 0, origin, UP).wait_recv()

                    @pl.when(can_up)
                    def _():
                        copy(kind, 0, origin, UP).start()

                @pl.when(above < nz)
                def _():
                    origin = above * 2 + column
                    copy(kind, 0, origin, DOWN).wait_recv()

                    @pl.when(can_down)
                    def _():
                        copy(kind, 0, origin, DOWN).start()

    def wait_across(kind, origin):
        for part in rest_of(kind):
            copy(kind, part, origin, ACROSS).wait_recv()

    def drain(kind):
        def body(origin, carry):
            oz, ox = origin // 2, origin % 2
            for part in range(len(cuts[kind])):
                if not cuts[kind][part]:
                    continue
                mine = (ox == x) | (part == 0)

                @pl.when(mine & (oz <= z) & can_up)
                def _():
                    copy(kind, part, origin, UP).wait_send()

                @pl.when(mine & (oz >= z) & can_down)
                def _():
                    copy(kind, part, origin, DOWN).wait_send()

                @pl.when((origin == me) if part == 0 else (ox == x))
                def _():
                    copy(kind, part, origin, ACROSS).wait_send()

            return carry

        lax.fori_loop(0, n_dp, body, 0)

    for load in loads[:3]:
        load.wait()
    send_own(0)

    total = jnp.zeros((local_len, 1), jnp.float32)
    for block in range(n_dp):
        rows = hid[:, block * fcols : (block + 1) * fcols].astype(jnp.float32)
        total = total + jnp.sum(rows * rows, axis=-1, keepdims=True)
    scale = lax.rsqrt(total / width + 1e-06)
    for block in range(n_dp):
        span = slice(block * fcols, (block + 1) * fcols)
        rows = hid[:, span].astype(jnp.float32)
        nbuf[mp, block] = (rows * scale * ngain[:, span]).astype(jnp.bfloat16)

    def share(step):
        return pltpu.make_async_remote_copy(
            src_ref=nbuf.at[mp],
            dst_ref=nbuf.at[mp],
            send_sem=nsend_sem.at[step],
            recv_sem=nrecv_sem.at[mp],
            device_id=(me, lax.rem(mp + step, n_mp)),
            device_id_type=MESH,
        )

    def shared(source):
        return pltpu.make_async_remote_copy(
            src_ref=nbuf.at[source],
            dst_ref=nbuf.at[source],
            send_sem=nsend_sem.at[0],
            recv_sem=nrecv_sem.at[source],
            device_id=(me, source),
            device_id_type=MESH,
        )

    for step in range(1, n_mp):
        share(step).start()
    send_partner(0)
    acc[...] = jnp.zeros_like(acc)

    def step_qkv(k, carry):
        relay(0, k)
        return carry

    lax.fori_loop(1, nz, step_qkv, 0)
    loads[3].wait()
    send_own(1)
    for step in range(1, n_mp):
        shared(lax.rem(mp + step, n_mp)).wait_recv()

    def project(i, carry):
        other, k, side = i // (2 * nz), i // 2 % nz, i % 2
        oz = z + k * (2 * side - 1)
        origin = oz * 2 + lax.rem(x + other, 2)

        @pl.when((oz >= 0) & (oz < nz) & ((side == 0) | (k > 0)))
        def _():
            @pl.when(other == 1)
            def _():
                wait_across(0, origin)

            for m in range(n_mp):
                span = slice(m * local_len, (m + 1) * local_len)
                acc[span, :] += jnp.dot(
                    nbuf[m, origin], wbuf[origin], preferred_element_type=jnp.float32
                )

        return carry

    lax.fori_loop(0, 4 * nz, project, 0)

    length = len_ref[0]
    live = lax.broadcasted_iota(jnp.int32, (maxlen, HD), 0) < length

    def rotated(block, span):
        return block * cos_ref[span, :] + pltpu.roll(block, HD // 2, 1) * sin_ref[span, :]

    everything = slice(0, maxlen)
    for h in range(kv_heads):
        cols = slice(h * HD, (h + 1) * HD)
        keys = rotated(acc[:, qw + h * HD : qw + (h + 1) * HD], everything)
        key_out[:, cols] = jnp.where(live, keys, 0.0).astype(jnp.bfloat16)
        values = acc[:, qw + kw + h * HD : qw + kw + (h + 1) * HD]
        val_out[:, cols] = jnp.where(live, values, 0.0).astype(jnp.bfloat16)
    for h in range(q_heads):
        if h == q_heads // 2:
            send_partner(1)
            relay(1, 1)
        kv = h * kv_heads // q_heads
        cols = slice(kv * HD, (kv + 1) * HD)
        for r in range(n_mp):
            span, seen = slice(r * local_len, (r + 1) * local_len), (r + 1) * local_len
            query = rotated(acc[span, h * HD : (h + 1) * HD], span) * 144.0 ** (-0.5)
            score = lax.dot_general(
                query.astype(jnp.bfloat16),
                key_out[:seen, cols],
                (((1,), (1,)), ((), ())),
                preferred_element_type=jnp.float32,
            )
            row = lax.broadcasted_iota(jnp.int32, score.shape, 0) + r * local_len
            col = lax.broadcasted_iota(jnp.int32, score.shape, 1)
            expo = jnp.exp(50.0 * jnp.tanh(score * (1.0 / 50.0)))
            expo = jnp.where((col <= row) & (col < length), expo, 0.0)
            weights = (expo / jnp.sum(expo, axis=-1, keepdims=True)).astype(jnp.bfloat16)
            att[span, h * HD : (h + 1) * HD] = jnp.dot(
                weights, val_out[:seen, cols], preferred_element_type=jnp.float32
            ).astype(jnp.bfloat16)

    def hand(block, step):
        target = lax.rem(mp + step, n_mp)
        return pltpu.make_async_remote_copy(
            src_ref=psend.at[block, target],
            dst_ref=precv.at[block, n_mp - 1 - step],
            send_sem=psend_sem.at[block, n_mp - 1 - step],
            recv_sem=precv_sem.at[block, n_mp - 1 - step],
            device_id=(me, target),
            device_id_type=MESH,
        )

    def output(block):
        for m in range(n_mp):
            span = slice(m * local_len, (m + 1) * local_len)
            psend[block, m] = jnp.dot(
                att[span, :], obuf[block], preferred_element_type=jnp.float32
            ).astype(jnp.bfloat16)
        for step in range(1, n_mp):
            hand(block, step).start()

    def step_out(k, carry):
        @pl.when((k > 1) & (k < nz))
        def _():
            relay(1, k)

        def each(i, inner):
            other, side = i // 2, i % 2
            distance = k - other
            oz = z + distance * (2 * side - 1)
            origin = oz * 2 + lax.rem(x + other, 2)

            @pl.when(
                (distance >= 0) & (distance < nz) & (oz >= 0) & (oz < nz)
                & ((side == 0) | (distance > 0))
            )
            def _():
                @pl.when(other == 1)
                def _():
                    wait_across(1, origin)

                output(origin)

            return inner

        return lax.fori_loop(0, 4, each, carry)

    lax.fori_loop(0, nz + 1, step_out, 0)

    def summed(block):
        value = psend[block, mp].astype(jnp.float32)
        for slot in range(n_mp - 1):
            value = value + precv[block, slot].astype(jnp.float32)
        return value

    def squares(block, total):
        for step in range(1, n_mp):
            hand(block, step).wait_recv()
        value = summed(block)
        return total + jnp.sum(value * value, axis=-1, keepdims=True)

    total = lax.fori_loop(0, n_dp, squares, jnp.zeros((local_len, 1), jnp.float32))
    scale = lax.rsqrt(total / width + 1e-06)
    own = lax.broadcasted_iota(jnp.int32, (local_len, fcols), 0) + mp * local_len < length
    for block in range(n_dp):
        span = slice(block * fcols, (block + 1) * fcols)
        post = summed(block) * scale * pgain[:, span]
        mixed[:, span] = jnp.where(own, hid[:, span].astype(jnp.float32) + post, 0.0).astype(
            jnp.bfloat16
        )

    drain(0)
    drain(1)
    for step in range(1, n_mp):
        share(step).wait_send()

    def drain_hand(block, carry):
        for step in range(1, n_mp):
            hand(block, step).wait_send()
        return carry

    lax.fori_loop(0, n_dp, drain_hand, 0)


def local(n_dp, n_mp, hidden, lengths, norm_gain, w_query, w_key, w_value, w_out, post_gain):
    _, local_len, width = hidden.shape
    maxlen = local_len * n_mp
    rows, qw = w_query.shape
    kw = w_key.shape[1]
    orows, fcols = w_out.shape
    cuts = (cut(rows), cut(orows))
    cosine, sine = tables(maxlen)
    vmem = pl.BlockSpec(memory_space=pltpu.VMEM)
    anywhere = pl.BlockSpec(memory_space=pl.ANY)
    bf16, f32 = jnp.bfloat16, jnp.float32
    dma = pltpu.SemaphoreType.DMA
    mixed, keys, values = pl.pallas_call(
        functools.partial(kernel, n_dp, n_mp, cuts),
        out_shape=(
            jax.ShapeDtypeStruct((local_len, width), bf16),
            jax.ShapeDtypeStruct((maxlen, kw), bf16),
            jax.ShapeDtypeStruct((maxlen, kw), bf16),
        ),
        in_specs=[pl.BlockSpec(memory_space=pltpu.SMEM), vmem, vmem]
        + [anywhere] * 4
        + [vmem, vmem, vmem],
        out_specs=(vmem, vmem, vmem),
        scratch_shapes=[
            pltpu.VMEM((n_dp, rows, qw + 2 * kw), bf16),
            pltpu.VMEM((n_dp, orows, fcols), bf16),
            pltpu.VMEM((n_mp, n_dp, local_len, fcols), bf16),
            pltpu.VMEM((maxlen, qw + 2 * kw), f32),
            pltpu.VMEM((maxlen, qw), bf16),
            pltpu.VMEM((n_dp, n_mp, local_len, fcols), bf16),
            pltpu.VMEM((n_dp, n_mp - 1, local_len, fcols), bf16),
            dma((4,)),
            dma((2, 3, 3, n_dp)),
            dma((2, 3, n_dp)),
            dma((n_mp,)),
            dma((n_mp,)),
            dma((n_dp, n_mp - 1)),
            dma((n_dp, n_mp - 1)),
        ],
        compiler_params=pltpu.CompilerParams(
            collective_id=0, has_side_effects=True, vmem_limit_bytes=60 * 1024 * 1024
        ),
    )(
        lengths,
        hidden[0],
        norm_gain.reshape(1, width),
        w_query,
        w_key,
        w_value,
        w_out,
        post_gain.reshape(1, width),
        jnp.asarray(cosine),
        jnp.asarray(sine),
    )
    return mixed[None], keys[None], values[None]


def solution(mesh):
    return jax.shard_map(
        functools.partial(local, mesh.shape["dp"], mesh.shape["mp"]),
        mesh=mesh,
        in_specs=(
            P("dp", "mp", None),
            P("dp"),
            P(),
            P("dp", "mp"),
            P("dp", "mp"),
            P("dp", "mp"),
            P("mp", "dp"),
            P(),
        ),
        out_specs=(P("dp", "mp", None), P("dp", None, "mp"), P("dp", None, "mp")),
        check_vma=False,
    )
```

```python
import functools

import jax
import jax.numpy as jnp
import numpy as np
from jax import lax
from jax.experimental import pallas as pl
from jax.experimental.pallas import tpu as pltpu
from jax.sharding import PartitionSpec as P

HD = 128
MESH = pl.DeviceIdType.MESH
UP, DOWN, ACROSS = 0, 1, 2


def tables(maxlen):
    half = HD // 2
    freqs = 10000.0 ** (-np.arange(half, dtype=np.float64) / half)
    angles = np.arange(maxlen, dtype=np.float64)[:, None] * freqs[None, :]
    cosine, sine = np.cos(angles), np.sin(angles)
    return (
        np.concatenate([cosine, cosine], axis=1).astype(np.float32),
        np.concatenate([-sine, sine], axis=1).astype(np.float32),
    )


def cut(rows):
    if rows % 32:
        return [None, (0, rows)]
    first = rows // 6 // 16 * 16
    rest = rows - first
    chunk = rest // 2 // 16 * 16
    return [(0, first), (first, chunk), (first + chunk, rest - chunk)]


def kernel(
    n_dp, n_mp, cuts,
    len_ref, hid, ngain, wq, wk, wv, wo, pgain, cos_ref, sin_ref,
    mixed, key_out, val_out,
    wbuf, obuf, nbuf, acc, att, psend, precv, inbox,
    load_sem, send_sem, recv_sem, nsend_sem, nrecv_sem, psend_sem, precv_sem, fsend_sem, inbox_sem,
):
    nz = n_dp // 2
    me, mp = lax.axis_index("dp"), lax.axis_index("mp")
    z, x = me // 2, me % 2
    local_len, width = hid.shape
    maxlen = local_len * n_mp
    fcols = width // n_dp
    qw, kw = wq.shape[1], wk.shape[1]
    q_heads, kv_heads = qw // HD, kw // HD
    can_up, can_down = z < nz - 1, z > 0
    bufs = (wbuf, obuf)

    loads = [
        pltpu.make_async_copy(wq, wbuf.at[me, :, pl.ds(0, qw)], load_sem.at[0]),
        pltpu.make_async_copy(wk, wbuf.at[me, :, pl.ds(qw, kw)], load_sem.at[1]),
        pltpu.make_async_copy(wv, wbuf.at[me, :, pl.ds(qw + kw, kw)], load_sem.at[2]),
        pltpu.make_async_copy(wo, obuf.at[me], load_sem.at[3]),
    ]
    for load in loads:
        load.start()

    barrier = pltpu.get_barrier_semaphore()

    def greet(dp_index, mp_index):
        pl.semaphore_signal(barrier, inc=1, device_id=(dp_index, mp_index), device_id_type=MESH)

    greet(me + 1 - 2 * x, mp)
    for step in range(1, n_mp):
        greet(me, lax.rem(mp + step, n_mp))

    @pl.when(can_up)
    def _():
        greet(me + 2, mp)

    @pl.when(can_down)
    def _():
        greet(me - 2, mp)

    pl.semaphore_wait(
        barrier, n_mp + jnp.where(can_up, 1, 0) + jnp.where(can_down, 1, 0)
    )

    def copy(kind, part, origin, way):
        start, size = cuts[kind][part]
        ref = bufs[kind].at[origin, pl.ds(start, size)]
        target = (me + 2, me - 2, me + 1 - 2 * x)[way]
        return pltpu.make_async_remote_copy(
            src_ref=ref,
            dst_ref=ref,
            send_sem=send_sem.at[kind, part, way, origin],
            recv_sem=recv_sem.at[kind, part, origin],
            device_id=(target, mp),
            device_id_type=MESH,
        )

    def send_chain(kind, part, origin):
        @pl.when(can_up)
        def _():
            copy(kind, part, origin, UP).start()

        @pl.when(can_down)
        def _():
            copy(kind, part, origin, DOWN).start()

    def rest_of(kind):
        return range(1, len(cuts[kind]))

    def send_own(kind):
        if cuts[kind][0]:
            copy(kind, 0, me, ACROSS).start()
        for part in rest_of(kind):
            send_chain(kind, part, me)
            copy(kind, part, me, ACROSS).start()
        if cuts[kind][0]:
            send_chain(kind, 0, me)

    def send_partner(kind):
        if cuts[kind][0]:
            partner = me + 1 - 2 * x
            copy(kind, 0, partner, ACROSS).wait_recv()
            send_chain(kind, 0, partner)

    def relay(kind, k):
        below, above = z - k, z + k
        for part in rest_of(kind):
            @pl.when(below >= 0)
            def _():
                origin = below * 2 + x
                copy(kind, part, origin, UP).wait_recv()

                @pl.when(can_up)
                def _():
                    copy(kind, part, origin, UP).start()

                copy(kind, part, origin, ACROSS).start()

            @pl.when(above < nz)
            def _():
                origin = above * 2 + x
                copy(kind, part, origin, DOWN).wait_recv()

                @pl.when(can_down)
                def _():
                    copy(kind, part, origin, DOWN).start()

                copy(kind, part, origin, ACROSS).start()

        if cuts[kind][0]:
            for column in range(2):
                @pl.when(below >= 0)
                def _():
                    origin = below * 2 + column
                    copy(kind, 0, origin, UP).wait_recv()

                    @pl.when(can_up)
                    def _():
                        copy(kind, 0, origin, UP).start()

                @pl.when(above < nz)
                def _():
                    origin = above * 2 + column
                    copy(kind, 0, origin, DOWN).wait_recv()

                    @pl.when(can_down)
                    def _():
                        copy(kind, 0, origin, DOWN).start()

    def wait_across(kind, origin):
        for part in rest_of(kind):
            copy(kind, part, origin, ACROSS).wait_recv()

    def drain(kind):
        def body(origin, carry):
            oz, ox = origin // 2, origin % 2
            for part in range(len(cuts[kind])):
                if not cuts[kind][part]:
                    continue
                mine = (ox == x) | (part == 0)

                @pl.when(mine & (oz <= z) & can_up)
                def _():
                    copy(kind, part, origin, UP).wait_send()

                @pl.when(mine & (oz >= z) & can_down)
                def _():
                    copy(kind, part, origin, DOWN).wait_send()

                @pl.when((origin == me) if part == 0 else (ox == x))
                def _():
                    copy(kind, part, origin, ACROSS).wait_send()

            return carry

        lax.fori_loop(0, n_dp, body, 0)

    for load in loads[:3]:
        load.wait()
    send_own(0)

    total = jnp.zeros((local_len, 1), jnp.float32)
    for block in range(n_dp):
        rows = hid[:, block * fcols : (block + 1) * fcols].astype(jnp.float32)
        total = total + jnp.sum(rows * rows, axis=-1, keepdims=True)
    scale = lax.rsqrt(total / width + 1e-06)
    for block in range(n_dp):
        span = slice(block * fcols, (block + 1) * fcols)
        rows = hid[:, span].astype(jnp.float32)
        nbuf[mp, block] = (rows * scale * ngain[:, span]).astype(jnp.bfloat16)

    def share(step):
        return pltpu.make_async_remote_copy(
            src_ref=nbuf.at[mp],
            dst_ref=nbuf.at[mp],
            send_sem=nsend_sem.at[step],
            recv_sem=nrecv_sem.at[mp],
            device_id=(me, lax.rem(mp + step, n_mp)),
            device_id_type=MESH,
        )

    def shared(source):
        return pltpu.make_async_remote_copy(
            src_ref=nbuf.at[source],
            dst_ref=nbuf.at[source],
            send_sem=nsend_sem.at[0],
            recv_sem=nrecv_sem.at[source],
            device_id=(me, source),
            device_id_type=MESH,
        )

    for step in range(1, n_mp):
        share(step).start()
    send_partner(0)
    acc[...] = jnp.zeros_like(acc)

    def step_qkv(k, carry):
        relay(0, k)
        return carry

    lax.fori_loop(1, nz, step_qkv, 0)
    loads[3].wait()
    send_own(1)
    for step in range(1, n_mp):
        shared(lax.rem(mp + step, n_mp)).wait_recv()

    def project(i, carry):
        other, k, side = i // (2 * nz), i // 2 % nz, i % 2
        oz = z + k * (2 * side - 1)
        origin = oz * 2 + lax.rem(x + other, 2)

        @pl.when((oz >= 0) & (oz < nz) & ((side == 0) | (k > 0)))
        def _():
            @pl.when(other == 1)
            def _():
                wait_across(0, origin)

            for m in range(n_mp):
                span = slice(m * local_len, (m + 1) * local_len)
                acc[span, :] += jnp.dot(
                    nbuf[m, origin], wbuf[origin], preferred_element_type=jnp.float32
                )

        return carry

    lax.fori_loop(0, 4 * nz, project, 0)
    send_partner(1)

    length = len_ref[0]
    live = lax.broadcasted_iota(jnp.int32, (maxlen, HD), 0) < length

    def rotated(block, span):
        return block * cos_ref[span, :] + pltpu.roll(block, HD // 2, 1) * sin_ref[span, :]

    everything = slice(0, maxlen)
    for h in range(kv_heads):
        cols = slice(h * HD, (h + 1) * HD)
        keys = rotated(acc[:, qw + h * HD : qw + (h + 1) * HD], everything)
        key_out[:, cols] = jnp.where(live, keys, 0.0).astype(jnp.bfloat16)
        values = acc[:, qw + kw + h * HD : qw + kw + (h + 1) * HD]
        val_out[:, cols] = jnp.where(live, values, 0.0).astype(jnp.bfloat16)
    for h in range(q_heads):
        kv = h * kv_heads // q_heads
        cols = slice(kv * HD, (kv + 1) * HD)
        for r in range(n_mp):
            span, seen = slice(r * local_len, (r + 1) * local_len), (r + 1) * local_len
            query = rotated(acc[span, h * HD : (h + 1) * HD], span) * 144.0 ** (-0.5)
            score = lax.dot_general(
                query.astype(jnp.bfloat16),
                key_out[:seen, cols],
                (((1,), (1,)), ((), ())),
                preferred_element_type=jnp.float32,
            )
            row = lax.broadcasted_iota(jnp.int32, score.shape, 0) + r * local_len
            col = lax.broadcasted_iota(jnp.int32, score.shape, 1)
            expo = jnp.exp(50.0 * jnp.tanh(score * (1.0 / 50.0)))
            expo = jnp.where((col <= row) & (col < length), expo, 0.0)
            weights = (expo / jnp.sum(expo, axis=-1, keepdims=True)).astype(jnp.bfloat16)
            att[span, h * HD : (h + 1) * HD] = jnp.dot(
                weights, val_out[:seen, cols], preferred_element_type=jnp.float32
            ).astype(jnp.bfloat16)

    pairs = n_mp // 2
    mate = mp + 1 - 2 * lax.rem(mp, 2)

    def hand(block, step):
        part = lax.rem(mate + 2 * step, n_mp)
        return pltpu.make_async_remote_copy(
            src_ref=psend.at[block, part],
            dst_ref=precv.at[block, 0] if step == 0 else inbox.at[block, step - 1],
            send_sem=psend_sem.at[block, step],
            recv_sem=precv_sem.at[block, 0] if step == 0 else inbox_sem.at[block, step - 1],
            device_id=(me, mate),
            device_id_type=MESH,
        )

    def far(block, step):
        target = lax.rem(mp + 2 * step, n_mp)
        return pltpu.make_async_remote_copy(
            src_ref=psend.at[block, target],
            dst_ref=precv.at[block, pairs - step],
            send_sem=fsend_sem.at[block, step - 1],
            recv_sem=precv_sem.at[block, pairs - step],
            device_id=(me, target),
            device_id_type=MESH,
        )

    def forward(block):
        for step in range(1, pairs):
            hand(block, step).wait_recv()
            target = lax.rem(mp + 2 * step, n_mp)
            both = psend[block, target].astype(jnp.float32) + inbox[block, step - 1].astype(
                jnp.float32
            )
            psend[block, target] = both.astype(jnp.bfloat16)
            far(block, step).start()

    def output(block):
        for m in range(n_mp):
            span = slice(m * local_len, (m + 1) * local_len)
            psend[block, m] = jnp.dot(
                att[span, :], obuf[block], preferred_element_type=jnp.float32
            ).astype(jnp.bfloat16)
        for step in list(range(1, pairs)) + [0]:
            hand(block, step).start()

    def step_out(k, carry):
        @pl.when((k > 0) & (k < nz))
        def _():
            relay(1, k)

        def each(i, inner):
            other, side = i // 2, i % 2
            distance = k - other
            oz = z + distance * (2 * side - 1)
            origin = oz * 2 + lax.rem(x + other, 2)

            @pl.when(
                (distance >= 0) & (distance < nz) & (oz >= 0) & (oz < nz)
                & ((side == 0) | (distance > 0))
            )
            def _():
                @pl.when(other == 1)
                def _():
                    wait_across(1, origin)

                output(origin)
                forward(origin)

            return inner

        return lax.fori_loop(0, 4, each, carry)

    lax.fori_loop(0, nz + 1, step_out, 0)

    def summed(block):
        value = psend[block, mp].astype(jnp.float32)
        for slot in range(pairs):
            value = value + precv[block, slot].astype(jnp.float32)
        return value

    def squares(block, total):
        hand(block, 0).wait_recv()
        for step in range(1, pairs):
            far(block, step).wait_recv()
        value = summed(block)
        return total + jnp.sum(value * value, axis=-1, keepdims=True)

    total = lax.fori_loop(0, n_dp, squares, jnp.zeros((local_len, 1), jnp.float32))
    scale = lax.rsqrt(total / width + 1e-06)
    own = lax.broadcasted_iota(jnp.int32, (local_len, fcols), 0) + mp * local_len < length
    for block in range(n_dp):
        span = slice(block * fcols, (block + 1) * fcols)
        post = summed(block) * scale * pgain[:, span]
        mixed[:, span] = jnp.where(own, hid[:, span].astype(jnp.float32) + post, 0.0).astype(
            jnp.bfloat16
        )

    drain(0)
    drain(1)
    for step in range(1, n_mp):
        share(step).wait_send()

    def drain_hand(block, carry):
        for step in range(pairs):
            hand(block, step).wait_send()
        for step in range(1, pairs):
            far(block, step).wait_send()
        return carry

    lax.fori_loop(0, n_dp, drain_hand, 0)


def local(n_dp, n_mp, hidden, lengths, norm_gain, w_query, w_key, w_value, w_out, post_gain):
    _, local_len, width = hidden.shape
    maxlen = local_len * n_mp
    rows, qw = w_query.shape
    kw = w_key.shape[1]
    orows, fcols = w_out.shape
    cuts = (cut(rows), cut(orows))
    cosine, sine = tables(maxlen)
    vmem = pl.BlockSpec(memory_space=pltpu.VMEM)
    anywhere = pl.BlockSpec(memory_space=pl.ANY)
    bf16, f32 = jnp.bfloat16, jnp.float32
    dma = pltpu.SemaphoreType.DMA
    mixed, keys, values = pl.pallas_call(
        functools.partial(kernel, n_dp, n_mp, cuts),
        out_shape=(
            jax.ShapeDtypeStruct((local_len, width), bf16),
            jax.ShapeDtypeStruct((maxlen, kw), bf16),
            jax.ShapeDtypeStruct((maxlen, kw), bf16),
        ),
        in_specs=[pl.BlockSpec(memory_space=pltpu.SMEM), vmem, vmem]
        + [anywhere] * 4
        + [vmem, vmem, vmem],
        out_specs=(vmem, vmem, vmem),
        scratch_shapes=[
            pltpu.VMEM((n_dp, rows, qw + 2 * kw), bf16),
            pltpu.VMEM((n_dp, orows, fcols), bf16),
            pltpu.VMEM((n_mp, n_dp, local_len, fcols), bf16),
            pltpu.VMEM((maxlen, qw + 2 * kw), f32),
            pltpu.VMEM((maxlen, qw), bf16),
            pltpu.VMEM((n_dp, n_mp, local_len, fcols), bf16),
            pltpu.VMEM((n_dp, n_mp // 2, local_len, fcols), bf16),
            pltpu.VMEM((n_dp, n_mp // 2 - 1, local_len, fcols), bf16),
            dma((4,)),
            dma((2, 3, 3, n_dp)),
            dma((2, 3, n_dp)),
            dma((n_mp,)),
            dma((n_mp,)),
            dma((n_dp, n_mp // 2)),
            dma((n_dp, n_mp // 2)),
            dma((n_dp, n_mp // 2 - 1)),
            dma((n_dp, n_mp // 2 - 1)),
        ],
        compiler_params=pltpu.CompilerParams(
            collective_id=0, has_side_effects=True, vmem_limit_bytes=60 * 1024 * 1024
        ),
    )(
        lengths,
        hidden[0],
        norm_gain.reshape(1, width),
        w_query,
        w_key,
        w_value,
        w_out,
        post_gain.reshape(1, width),
        jnp.asarray(cosine),
        jnp.asarray(sine),
    )
    return mixed[None], keys[None], values[None]


def solution(mesh):
    return jax.shard_map(
        functools.partial(local, mesh.shape["dp"], mesh.shape["mp"]),
        mesh=mesh,
        in_specs=(
            P("dp", "mp", None),
            P("dp"),
            P(),
            P("dp", "mp"),
            P("dp", "mp"),
            P("dp", "mp"),
            P("mp", "dp"),
            P(),
        ),
        out_specs=(P("dp", "mp", None), P("dp", None, "mp"), P("dp", None, "mp")),
        check_vma=False,
    )
```
